32 devices in a mesh: dpz: 4 (over z), dpy: 2 (over y), dpx: 4 (over x, core).
Axes of the slice: x: 2, y: 2, z: 4, core: 2. Of those that a mesh axis runs over, the one named last changes fastest.
Arguments:
- x_in: bfloat16 [98304, 1024], P(('dpz', 'dpy', 'dpx'))
- dy_out: bfloat16 [98304, 1024], P(('dpz', 'dpy', 'dpx'))
- w1_in: bfloat16 [1024, 2816], replicated
- w1_out: bfloat16 [2816, 1024], replicated
- w2_in: bfloat16 [1024, 2816], replicated
- w2_out: bfloat16 [2816, 1024], replicated
- master: float32 [11534336], P(('dpz', 'dpy', 'dpx'))
- adam_m: float32 [11534336], P(('dpz', 'dpy', 'dpx'))
- adam_v: float32 [11534336], P(('dpz', 'dpy', 'dpx'))
Outputs:
- output 1: float32 [11534336], P(('dpz', 'dpy', 'dpx'))
- output 2: float32 [11534336], P(('dpz', 'dpy', 'dpx'))
- output 3: float32 [11534336], P(('dpz', 'dpy', 'dpx'))
- output 4: bfloat16 [11534336], replicated
All inputs are finite; a program needn't handle non-finite values.
Results may differ from the reference program's by a relative error of at most 0.00926145.
Values are sent between devices in bfloat16 or wider.
A program may use at most 1 GiB of HBM per device.

```python
import math
import jax
import jax.numpy as jnp
from jax import lax

D = 1024
FF = 2816
TOKENS = 3072
NDEV = 32
STEP = 10

BETA_ONE = 0.9
BETA_TWO = 0.999
LEARN_RATE = 0.001
ADAM_EPS = 1e-8


def gelu_value(z_val):
    return 0.5 * z_val * (1.0 + lax.erf(z_val * (1.0 / math.sqrt(2.0))))


def gelu_slope(z_val):
    cdf_part = 0.5 * (1.0 + lax.erf(z_val * (1.0 / math.sqrt(2.0))))
    return cdf_part + z_val * jnp.exp(-0.5 * z_val * z_val) * (1.0 / math.sqrt(2.0 * math.pi))


def setup_inputs(seed: int = 0) -> dict:
    key_list = jax.random.split(jax.random.key(seed), 9)
    total_len = 4 * D * FF
    row_count = NDEV * TOKENS
    grad_scale = math.sqrt(row_count)
    act_vals = jax.random.normal(key_list[0], (row_count, D), jnp.float32)
    out_grad = jax.random.normal(key_list[1], (row_count, D), jnp.float32)
    w1_in = jax.random.normal(key_list[2], (D, FF), jnp.float32) * D ** -0.5
    w1_out = jax.random.normal(key_list[3], (FF, D), jnp.float32) * FF ** -0.5
    w2_in = jax.random.normal(key_list[4], (D, FF), jnp.float32) * D ** -0.5
    w2_out = jax.random.normal(key_list[5], (FF, D), jnp.float32) * FF ** -0.5
    master = jax.random.normal(key_list[6], (total_len,), jnp.float32) * 0.02
    adam_m = jax.random.normal(key_list[7], (total_len,), jnp.float32) * (0.05 * grad_scale)
    adam_v = jax.random.uniform(key_list[8], (total_len,), jnp.float32, 0.5, 1.5) * (0.0004 * row_count)
    return {'x_in': act_vals.astype(jnp.bfloat16), 'dy_out': out_grad.astype(jnp.bfloat16), 'w1_in': w1_in.astype(jnp.bfloat16), 'w1_out': w1_out.astype(jnp.bfloat16), 'w2_in': w2_in.astype(jnp.bfloat16), 'w2_out': w2_out.astype(jnp.bfloat16), 'master': master, 'adam_m': adam_m, 'adam_v': adam_v}


def device_grads(x_one, dy_one, w1_in, w1_out, w2_in, w2_out):
    z_one = jnp.dot(x_one, w1_in, preferred_element_type=jnp.float32).astype(jnp.bfloat16)
    h_one = gelu_value(z_one.astype(jnp.float32)).astype(jnp.bfloat16)
    x_two = (x_one.astype(jnp.float32) + jnp.dot(h_one, w1_out, preferred_element_type=jnp.float32)).astype(jnp.bfloat16)
    z_two = jnp.dot(x_two, w2_in, preferred_element_type=jnp.float32).astype(jnp.bfloat16)
    h_two = gelu_value(z_two.astype(jnp.float32)).astype(jnp.bfloat16)
    g2_out = jnp.dot(h_two.T, dy_one, preferred_element_type=jnp.float32).astype(jnp.bfloat16)
    dz_two = (jnp.dot(dy_one, w2_out.T, preferred_element_type=jnp.float32) * gelu_slope(z_two.astype(jnp.float32))).astype(jnp.bfloat16)
    g2_in = jnp.dot(x_two.T, dz_two, preferred_element_type=jnp.float32).astype(jnp.bfloat16)
    dx_two = (dy_one.astype(jnp.float32) + jnp.dot(dz_two, w2_in.T, preferred_element_type=jnp.float32)).astype(jnp.bfloat16)
    g1_out = jnp.dot(h_one.T, dx_two, preferred_element_type=jnp.float32).astype(jnp.bfloat16)
    dz_one = (jnp.dot(dx_two, w1_out.T, preferred_element_type=jnp.float32) * gelu_slope(z_one.astype(jnp.float32))).astype(jnp.bfloat16)
    g1_in = jnp.dot(x_one.T, dz_one, preferred_element_type=jnp.float32).astype(jnp.bfloat16)
    return jnp.concatenate([g2_out.reshape(-1), g2_in.reshape(-1), g1_out.reshape(-1), g1_in.reshape(-1)])


def adam_update(master, adam_m, adam_v, grad_sum):
    new_m = BETA_ONE * adam_m + (1.0 - BETA_ONE) * grad_sum
    new_v = BETA_TWO * adam_v + (1.0 - BETA_TWO) * grad_sum * grad_sum
    m_hat = new_m / (1.0 - BETA_ONE ** STEP)
    v_hat = new_v / (1.0 - BETA_TWO ** STEP)
    new_master = master - LEARN_RATE * m_hat / (jnp.sqrt(v_hat) + ADAM_EPS)
    return new_master, new_m, new_v


def reference(x_in, dy_out, w1_in, w1_out, w2_in, w2_out, master, adam_m, adam_v):
    x_dev = x_in.reshape(NDEV, TOKENS, D)
    dy_dev = dy_out.reshape(NDEV, TOKENS, D)

    def accumulate(run_sum, dev_pair):
        grads = device_grads(dev_pair[0], dev_pair[1], w1_in, w1_out, w2_in, w2_out)
        return run_sum + grads.astype(jnp.float32), None

    start_sum = jnp.zeros((4 * D * FF,), jnp.float32)
    grad_sum = lax.scan(accumulate, start_sum, (x_dev, dy_dev))[0]
    new_master, new_m, new_v = adam_update(master, adam_m, adam_v, grad_sum)
    return (new_master, new_m, new_v, new_master.astype(jnp.bfloat16))
```

```python
import math
import jax
import jax.numpy as jnp
from jax import lax
from jax.sharding import PartitionSpec as P

AXES = ('dpz', 'dpy', 'dpx')
PLANE = ('dpy', 'dpx')
STEP = 10
BETA_ONE = 0.9
BETA_TWO = 0.999
LEARN_RATE = 0.001
ADAM_EPS = 1e-8


def gelu_value(z_val):
    return 0.5 * z_val * (1.0 + lax.erf(z_val * (1.0 / math.sqrt(2.0))))


def gelu_slope(z_val):
    cdf_part = 0.5 * (1.0 + lax.erf(z_val * (1.0 / math.sqrt(2.0))))
    return cdf_part + z_val * jnp.exp(-0.5 * z_val * z_val) * (1.0 / math.sqrt(2.0 * math.pi))


def round_wide(val):
    return lax.reduce_precision(val, 8, 7)


def plane_sum(grad_wide):
    return lax.psum_scatter(grad_wide, PLANE, scatter_dimension=0, tiled=True).reshape(-1)


def adam_step(master, adam_m, adam_v, grad_sum):
    new_m = BETA_ONE * adam_m + (1.0 - BETA_ONE) * grad_sum
    new_v = BETA_TWO * adam_v + (1.0 - BETA_TWO) * grad_sum * grad_sum
    m_hat = new_m / (1.0 - BETA_ONE ** STEP)
    v_hat = new_v / (1.0 - BETA_TWO ** STEP)
    return master - LEARN_RATE * m_hat / (jnp.sqrt(v_hat) + ADAM_EPS), new_m, new_v


def solution(mesh):
    depth = mesh.shape['dpz']

    def local_step(x_one, dy_one, w1_in, w1_out, w2_in, w2_out, master, adam_m, adam_v):
        f32, b16 = jnp.float32, jnp.bfloat16
        here = lax.axis_index('dpz')

        def to_owner(part, owner):
            total = part
            for step in range(1, depth):
                total = total + lax.ppermute(part, 'dpz', [((owner + step) % depth, owner)])
            return total

        z_one = jnp.dot(x_one, w1_in, preferred_element_type=f32).astype(b16)
        z_one, h_one = lax.optimization_barrier((z_one, gelu_value(z_one.astype(f32)).astype(b16)))
        x_two = (x_one.astype(f32) + jnp.dot(h_one, w1_out, preferred_element_type=f32)).astype(b16)
        z_two = jnp.dot(x_two, w2_in, preferred_element_type=f32).astype(b16)
        h_two = gelu_value(z_two.astype(f32)).astype(b16)
        grad_a = round_wide(jnp.einsum('tf,td->fd', h_two, dy_one, preferred_element_type=f32))
        grad_a, dy_one, z_two = lax.optimization_barrier((grad_a, dy_one, z_two))
        part_a = plane_sum(grad_a)
        dz_two = (jnp.einsum('td,fd->tf', dy_one, w2_out, preferred_element_type=f32) * gelu_slope(z_two.astype(f32))).astype(b16)
        dx_two = (dy_one.astype(f32) + jnp.einsum('tf,df->td', dz_two, w2_in, preferred_element_type=f32)).astype(b16)
        grad_c = round_wide(jnp.einsum('tf,td->fd', h_one, dx_two, preferred_element_type=f32))
        grad_c, dx_two = lax.optimization_barrier((grad_c, dx_two))
        part_c = plane_sum(grad_c)
        dz_one = (jnp.einsum('td,fd->tf', dx_two, w1_out, preferred_element_type=f32) * gelu_slope(z_one.astype(f32))).astype(b16)
        grad_d = round_wide(jnp.einsum('td,tf->df', x_one, dz_one, preferred_element_type=f32))
        grad_d, dz_two, part_a = lax.optimization_barrier((grad_d, dz_two, part_a))
        half = dz_two.shape[1] // 2
        grad_b = [round_wide(jnp.einsum('td,tf->df', x_two, cols, preferred_element_type=f32))
                  for cols in (dz_two[:, :half], dz_two[:, half:])]
        total_a = to_owner(part_a, 0)
        grad_d, part_c, total_a = lax.optimization_barrier((grad_d, part_c, total_a))
        part_d = plane_sum(grad_d)
        total_c = to_owner(part_c, 2)
        left, right, part_d, total_c = lax.optimization_barrier((*grad_b, part_d, total_c))
        part_left = plane_sum(left)
        part_right = plane_sum(right)
        far_d = [lax.ppermute(part_d, 'dpz', [(source, depth - 1)]) for source in range(depth - 2)]
        part_left, *far_d = lax.optimization_barrier((part_left, *far_d))
        total_d = sum(far_d, part_d + lax.ppermute(part_d, 'dpz', [(depth - 2, depth - 1)]))
        halves = [to_owner(part, 1).reshape(-1, half) for part in (part_left, part_right)]
        total_b = jnp.concatenate(halves, axis=1).reshape(-1)
        own_sum = total_a
        for owner, total in ((1, total_b), (2, total_c), (3, total_d)):
            own_sum = jnp.where(here == owner, total, own_sum)
        new_master, new_m, new_v = adam_step(master, adam_m, adam_v, own_sum)
        weights_bf = lax.all_gather(new_master.astype(b16), AXES, tiled=True)
        return new_master, new_m, new_v, weights_bf

    in_specs = (P(AXES, None), P(AXES, None), P(), P(), P(), P(), P(AXES), P(AXES), P(AXES))
    out_specs = (P(AXES), P(AXES), P(AXES), P())
    return jax.shard_map(local_step, mesh=mesh, in_specs=in_specs, out_specs=out_specs, check_vma=False)
```
